16 devices in a mesh: dp: 2 (over y, z), cp: 8 (over x, core).
Axes of the slice: x: 4, y: 2, z: 1, core: 2. Of those that a mesh axis runs over, the one named last changes fastest.
The devices are a block of a 4x4x8 slice.
Arguments:
- hidden: bfloat16 [16384, 2560], P(('dp', 'cp')), parts along dimension 0
- w_query: bfloat16 [6, 2560, 8, 256], replicated
- w_key: bfloat16 [6, 2560, 8, 256], replicated
- w_value: bfloat16 [6, 2560, 8, 256], replicated
- w_out: bfloat16 [6, 8, 256, 2560], replicated
Outputs:
- output: bfloat16 [16384, 2560], P(('dp', 'cp')), parts along dimension 0
There are 2 independent parts. The reference program is written for one: setup_inputs(seed, part) draws one part's arguments, and reference() takes and returns one part's arrays. A program takes and returns all parts, laid end to end along the dimension named above; an argument that names none is the same for every part.
All inputs are finite; a program needn't handle non-finite values.
Results may differ from the reference program's by a relative error of at most 0.0121398.
Values are sent between devices in bfloat16 or wider.
A program may use at most 768 MiB of HBM per device.

```python
import jax
import jax.numpy as jnp
from jax import lax

CP_SIZE = 8
TOK_DEV = 1024
D_MODEL = 2560
N_HEADS = 8
HEAD_DIM = 256
WINDOW = 1024
LAYERS = 6
SEQ = CP_SIZE * TOK_DEV
N_BACK = min((WINDOW + TOK_DEV - 2) // TOK_DEV, CP_SIZE - 1)
NORM_EPS = 1e-6
NEG_BIG = -1e30


def setup_inputs(seed: int = 0, part: int = 0) -> dict:
    rng_key = jax.random.key(seed)
    part_key = jax.random.fold_in(jax.random.fold_in(rng_key, 1), part)
    keys_w = jax.random.split(jax.random.fold_in(rng_key, 2), 4)
    width = N_HEADS * HEAD_DIM
    out_gain = jnp.where(jnp.arange(LAYERS) == LAYERS - 1, 4.0, 2.0).reshape(LAYERS, 1, 1, 1)
    in_shape = (LAYERS, D_MODEL, N_HEADS, HEAD_DIM)
    hidden = jax.random.normal(part_key, (SEQ, D_MODEL), jnp.float32)
    w_query = jax.random.normal(keys_w[0], in_shape, jnp.float32) * (1.2 * D_MODEL ** -0.5)
    w_key = jax.random.normal(keys_w[1], in_shape, jnp.float32) * D_MODEL ** -0.5
    w_value = jax.random.normal(keys_w[2], in_shape, jnp.float32) * D_MODEL ** -0.5
    w_out = jax.random.normal(keys_w[3], (LAYERS, N_HEADS, HEAD_DIM, D_MODEL), jnp.float32) * out_gain * width ** -0.5
    return {"hidden": hidden.astype(jnp.bfloat16), "w_query": w_query.astype(jnp.bfloat16), "w_key": w_key.astype(jnp.bfloat16), "w_value": w_value.astype(jnp.bfloat16), "w_out": w_out.astype(jnp.bfloat16)}


def rms_norm(hidden):
    hid_f = hidden.astype(jnp.float32)
    return (hid_f * lax.rsqrt(jnp.mean(hid_f * hid_f, axis=-1, keepdims=True) + NORM_EPS)).astype(jnp.bfloat16)


def project(normed, weight):
    flat_w = weight.reshape(D_MODEL, N_HEADS * HEAD_DIM)
    flat_out = jnp.dot(normed, flat_w, preferred_element_type=jnp.float32)
    return flat_out.astype(jnp.bfloat16).reshape(SEQ, N_HEADS, HEAD_DIM)


def empty_state():
    return (jnp.full((TOK_DEV, N_HEADS), NEG_BIG, jnp.float32), jnp.zeros((TOK_DEV, N_HEADS), jnp.float32), jnp.zeros((TOK_DEV, N_HEADS, HEAD_DIM), jnp.float32))


def block_update(soft_state, q_blk, k_blk, v_blk, allowed):
    run_max, run_sum, acc_out = soft_state
    scores = jnp.einsum("qhd,khd->qhk", q_blk.astype(jnp.float32), k_blk.astype(jnp.float32)) * HEAD_DIM ** -0.5
    scores = jnp.where(allowed, scores, NEG_BIG)
    new_max = jnp.maximum(run_max, jnp.max(scores, axis=-1))
    prob_blk = jnp.where(allowed, jnp.exp(scores - new_max[..., None]), 0.0)
    rescale = jnp.exp(run_max - new_max)
    new_sum = run_sum * rescale + jnp.sum(prob_blk, axis=-1)
    prob_low = prob_blk.astype(jnp.bfloat16).astype(jnp.float32)
    new_acc = acc_out * rescale[..., None] + jnp.einsum("qhk,khd->qhd", prob_low, v_blk.astype(jnp.float32))
    return new_max, new_sum, new_acc


def finish(soft_state):
    run_max, run_sum, acc_out = soft_state
    return (acc_out / run_sum[..., None]).astype(jnp.bfloat16)


def local_attention(q_all, k_all, v_all):
    q_blocks = q_all.reshape(CP_SIZE, TOK_DEV, N_HEADS, HEAD_DIM)
    zero_pad = jnp.zeros((N_BACK * TOK_DEV, N_HEADS, HEAD_DIM), k_all.dtype)
    k_blocks = jnp.concatenate([zero_pad, k_all], axis=0).reshape(CP_SIZE + N_BACK, TOK_DEV, N_HEADS, HEAD_DIM)
    v_blocks = jnp.concatenate([zero_pad, v_all], axis=0).reshape(CP_SIZE + N_BACK, TOK_DEV, N_HEADS, HEAD_DIM)
    offsets = jnp.arange(TOK_DEV)

    def one_block(q_args):
        q_blk, blk_idx = q_args
        q_pos = blk_idx * TOK_DEV + offsets
        soft_state = empty_state()
        for back_idx in range(N_BACK + 1):
            k_blk = lax.dynamic_index_in_dim(k_blocks, blk_idx + N_BACK - back_idx, 0, keepdims=False)
            v_blk = lax.dynamic_index_in_dim(v_blocks, blk_idx + N_BACK - back_idx, 0, keepdims=False)
            k_pos = (blk_idx - back_idx) * TOK_DEV + offsets
            pos_gap = q_pos[:, None] - k_pos[None, :]
            allowed = (pos_gap >= 0) & (pos_gap < WINDOW) & (k_pos[None, :] >= 0)
            soft_state = block_update(soft_state, q_blk, k_blk, v_blk, allowed[:, None, :])
        return finish(soft_state)

    attn_out = lax.map(one_block, (q_blocks, jnp.arange(CP_SIZE)))
    return attn_out.reshape(SEQ, N_HEADS, HEAD_DIM)


def global_attention(q_all, k_all, v_all):
    q_blocks = q_all.reshape(CP_SIZE, TOK_DEV, N_HEADS, HEAD_DIM)
    k_blocks = k_all.reshape(CP_SIZE, TOK_DEV, N_HEADS, HEAD_DIM)
    v_blocks = v_all.reshape(CP_SIZE, TOK_DEV, N_HEADS, HEAD_DIM)
    offsets = jnp.arange(TOK_DEV)

    def one_block(q_args):
        q_blk, blk_idx = q_args
        q_pos = blk_idx * TOK_DEV + offsets

        def key_step(soft_state, kv_args):
            k_blk, v_blk, kb_idx = kv_args
            k_pos = kb_idx * TOK_DEV + offsets
            allowed = k_pos[None, :] <= q_pos[:, None]
            return block_update(soft_state, q_blk, k_blk, v_blk, allowed[:, None, :]), None

        soft_state, unused_out = lax.scan(key_step, empty_state(), (k_blocks, v_blocks, jnp.arange(CP_SIZE)))
        return finish(soft_state)

    attn_out = lax.map(one_block, (q_blocks, jnp.arange(CP_SIZE)))
    return attn_out.reshape(SEQ, N_HEADS, HEAD_DIM)


def attn_layer(hidden, w_query, w_key, w_value, w_out, attend):
    normed = rms_norm(hidden)
    attn_out = attend(project(normed, w_query), project(normed, w_key), project(normed, w_value))
    out_proj = jnp.dot(attn_out.reshape(SEQ, N_HEADS * HEAD_DIM), w_out.reshape(N_HEADS * HEAD_DIM, D_MODEL), preferred_element_type=jnp.float32)
    return (hidden.astype(jnp.float32) + out_proj).astype(jnp.bfloat16)


def reference(hidden, w_query, w_key, w_value, w_out):
    def local_step(hid_state, layer_w):
        return attn_layer(hid_state, layer_w[0], layer_w[1], layer_w[2], layer_w[3], local_attention), None

    last = LAYERS - 1
    hidden, unused_out = lax.scan(local_step, hidden, (w_query[:last], w_key[:last], w_value[:last], w_out[:last]))
    return attn_layer(hidden, w_query[last], w_key[last], w_value[last], w_out[last], global_attention)
```

```python
import functools
import math

import jax
import jax.numpy as jnp
from jax import lax
from jax.experimental import pallas as pl
from jax.experimental.pallas import tpu as pltpu
from jax.sharding import PartitionSpec as P

WINDOW = 1024
NORM_EPS = 1e-6
NEG_BIG = -1e30
Q_ROWS = 256
G_ROWS = 512
N_COLS = 512
NORM_ROWS = 16
BF16 = jnp.bfloat16
F32 = jnp.float32
NT_DIMS = (((1,), (1,)), ((), ()))


def dot_nt(lhs, rhs):
    return lax.dot_general(lhs, rhs, NT_DIMS, preferred_element_type=F32)


def dot_nn(lhs, rhs):
    return jnp.dot(lhs, rhs, preferred_element_type=F32)


def aligned(start, size):
    return pl.ds(pl.multiple_of(start, size), size)


def norm_into(src_ref, src_row, dst_ref, dst_row, n_rows):
    def body(idx, carry):
        part = src_ref[pl.ds(pl.multiple_of(src_row + idx * NORM_ROWS, NORM_ROWS), NORM_ROWS), :].astype(F32)
        scale = lax.rsqrt(jnp.mean(part * part, axis=-1, keepdims=True) + NORM_EPS)
        dst_ref[pl.ds(pl.multiple_of(dst_row + idx * NORM_ROWS, NORM_ROWS), NORM_ROWS), :] = (part * scale).astype(BF16)
        return carry

    lax.fori_loop(0, n_rows // NORM_ROWS, body, 0, unroll=4)


def local_layers(n_cp, n_run, dims, x_hbm, wq_hbm, wk_hbm, wv_hbm, wo_hbm, out_hbm,
                 x_ref, halo, normed, qo, keys, vals, w_own, w_halo, w_out,
                 io_sem, own_sem, halo_sem, out_sem, send_sem, recv_sem, free_sem):
    n_tok, d_model, n_heads, head_dim = dims
    half = n_tok // 2
    n_cols = d_model // N_COLS
    exp_scale = head_dim ** -0.5 * math.log2(math.e)
    me = lax.axis_index("cp")
    right, left = lax.rem(me + 1, n_cp), lax.rem(me + n_cp - 1, n_cp)
    w_in = (wq_hbm, wk_hbm, wv_hbm)

    def own_copy(layer, head, slot, which):
        return pltpu.make_async_copy(w_in[which].at[layer, head], w_own.at[slot, which], own_sem.at[slot, which])

    def halo_copy(layer, head, slot, which):
        return pltpu.make_async_copy(w_in[which + 1].at[layer, head], w_halo.at[slot, which], halo_sem.at[slot, which])

    def out_copy(layer, col, slot):
        return pltpu.make_async_copy(wo_hbm.at[layer, :, aligned(col * N_COLS, N_COLS)], w_out.at[slot], out_sem.at[slot])

    def shift_copy(chunk):
        rows = pl.ds(pl.multiple_of((1 - chunk) * half, half), half)
        return pltpu.make_async_remote_copy(src_ref=x_ref.at[rows], dst_ref=halo.at[rows], send_sem=send_sem.at[chunk],
                                            recv_sem=recv_sem.at[chunk], device_id={"cp": right},
                                            device_id_type=pl.DeviceIdType.MESH)

    barrier = pltpu.get_barrier_semaphore()
    for neighbour in (left, right):
        pl.semaphore_signal(barrier, inc=1, device_id={"cp": neighbour}, device_id_type=pl.DeviceIdType.MESH)
    load = pltpu.make_async_copy(x_hbm, x_ref, io_sem)
    load.start()
    for which in range(3):
        own_copy(0, 0, 0, which).start()
    load.wait()
    pl.semaphore_wait(barrier, 2)
    for chunk in range(2):
        shift_copy(chunk).start()

    row_id = lax.broadcasted_iota(jnp.int32, (Q_ROWS, Q_ROWS), 0)
    col_id = lax.broadcasted_iota(jnp.int32, (Q_ROWS, Q_ROWS), 1)

    def attend(q_blk, cols):
        q_rows = aligned(q_blk * Q_ROWS, Q_ROWS)
        k_rows = pl.ds(pl.multiple_of(q_blk * Q_ROWS, Q_ROWS), WINDOW + Q_ROWS)
        scores = dot_nt(qo[q_rows, cols], keys[k_rows, cols])
        n_blk = WINDOW // Q_ROWS
        parts = [scores[:, blk * Q_ROWS:(blk + 1) * Q_ROWS] for blk in range(n_blk + 1)]
        parts[0] = jnp.where(col_id > row_id, parts[0], NEG_BIG)
        parts[n_blk] = jnp.where(col_id <= row_id, parts[n_blk], NEG_BIG)
        for blk in range(n_blk):
            parts[blk] = jnp.where((me > 0) | (q_blk + blk >= n_blk), parts[blk], NEG_BIG)
        top = functools.reduce(jnp.maximum, parts)
        top = jnp.max(top, axis=-1, keepdims=True)
        probs = [jnp.exp2((part - top) * exp_scale) for part in parts]
        total = jnp.sum(functools.reduce(jnp.add, probs), axis=-1, keepdims=True)
        weights = jnp.concatenate([prob.astype(BF16) for prob in probs], axis=1)
        qo[q_rows, cols] = (dot_nn(weights, vals[k_rows, cols]) / total).astype(BF16)

    def layer_step(layer, carry):
        norm_into(x_ref, 0, normed, 0, n_tok)
        for which in range(2):
            halo_copy(layer, 0, 0, which).start()

        def own_step(head, inner):
            slot = lax.rem(head, 2)

            @pl.when(head + 1 < n_heads)
            def _():
                for which in range(3):
                    own_copy(layer, head + 1, 1 - slot, which).start()

            cols = aligned(head * head_dim, head_dim)
            for which, (dst, base) in enumerate(((qo, 0), (keys, n_tok), (vals, n_tok))):
                own_copy(layer, head, slot, which).wait()
                for part in range(2):
                    dst[pl.ds(base + part * half, half), cols] = dot_nn(
                        normed[pl.ds(part * half, half), :], w_own[slot, which]).astype(BF16)
            return inner

        lax.fori_loop(0, n_heads, own_step, 0)

        def chunk_step(chunk, inner):
            row0 = pl.multiple_of((1 - chunk) * half, half)
            rows = pl.ds(row0, half)
            shift_copy(chunk).wait_recv()
            norm_into(halo, row0, normed, 0, half)

            @pl.when(layer + 1 < n_run)
            def _():
                pl.semaphore_signal(free_sem.at[chunk], inc=1, device_id={"cp": left}, device_id_type=pl.DeviceIdType.MESH)

            out_copy(layer, 0, 0).start()

            def head_step(head, deep):
                slot = lax.rem(head, 2)

                @pl.when(head + 1 < n_heads)
                def _():
                    for which in range(2):
                        halo_copy(layer, head + 1, 1 - slot, which).start()

                @pl.when((head + 1 == n_heads) & (chunk == 0))
                def _():
                    for which in range(2):
                        halo_copy(layer, 0, 1 - slot, which).start()

                @pl.when((head + 1 == n_heads) & (chunk == 1) & (layer + 1 < n_run))
                def _():
                    for which in range(3):
                        own_copy(layer + 1, 0, 0, which).start()

                cols = aligned(head * head_dim, head_dim)
                for which, dst in enumerate((keys, vals)):
                    halo_copy(layer, head, slot, which).wait()
                    dst[rows, cols] = dot_nn(normed[pl.ds(0, half), :], w_halo[slot, which]).astype(BF16)
                for sub in range(half // Q_ROWS):
                    attend((1 - chunk) * (half // Q_ROWS) + sub, cols)
                return deep

            lax.fori_loop(0, n_heads, head_step, 0)
            shift_copy(chunk).wait_send()

            def col_step(col, deep):
                slot = lax.rem(col, 2)

                @pl.when(col + 1 < n_cols)
                def _():
                    out_copy(layer, col + 1, 1 - slot).start()

                out_copy(layer, col, slot).wait()
                cols = aligned(col * N_COLS, N_COLS)
                x_ref[rows, cols] = (x_ref[rows, cols].astype(F32) + dot_nn(qo[rows, :], w_out[slot])).astype(BF16)
                return deep

            lax.fori_loop(0, n_cols, col_step, 0)

            @pl.when(layer + 1 < n_run)
            def _():
                pl.semaphore_wait(free_sem.at[chunk], 1)
                shift_copy(chunk).start()

            return inner

        lax.fori_loop(0, 2, chunk_step, 0)
        return carry

    lax.fori_loop(0, n_run, layer_step, 0)
    store = pltpu.make_async_copy(x_ref, out_hbm, io_sem)
    store.start()
    store.wait()


def global_layer(n_cp, layer, offsets, dims, x_hbm, wq_hbm, wk_hbm, wv_hbm, wo_hbm, out_hbm,
                 x_ref, normed, stage, held, o_stage, o_all, w_own, w_out, run_max, run_sum, acc,
                 io_sem, own_sem, out_sem, send_sem, recv_sem, o_send, o_recv):
    n_tok, d_model, n_heads, head_dim = dims
    half = n_tok // 2
    n_cols = d_model // N_COLS
    exp_scale = head_dim ** -0.5 * math.log2(math.e)
    me = lax.axis_index("cp")
    w_in = (wq_hbm, wk_hbm, wv_hbm)

    def peer(step):
        shift = jnp.int32(0)
        for idx, offset in enumerate(offsets):
            shift = jnp.where(step == idx, offset, shift)
        return lax.rem(me + shift, n_cp)

    def own_copy(head, slot, which):
        return pltpu.make_async_copy(w_in[which].at[layer, head], w_own.at[slot, which], own_sem.at[slot, which])

    def out_copy(col, slot):
        return pltpu.make_async_copy(wo_hbm.at[layer, :, aligned(col * N_COLS, N_COLS)], w_out.at[slot], out_sem.at[slot])

    def give_copy(dst):
        return pltpu.make_async_remote_copy(src_ref=stage.at[dst], dst_ref=held.at[me], send_sem=send_sem.at[dst],
                                            recv_sem=recv_sem.at[me], device_id={"cp": dst},
                                            device_id_type=pl.DeviceIdType.MESH)

    def take_wait(src):
        pltpu.make_async_remote_copy(src_ref=held.at[src], dst_ref=held.at[src], send_sem=send_sem.at[src],
                                     recv_sem=recv_sem.at[src], device_id={"cp": src},
                                     device_id_type=pl.DeviceIdType.MESH).wait_recv()

    my_cols = aligned(me * head_dim, head_dim)

    def back_copy(dst):
        return pltpu.make_async_remote_copy(src_ref=o_stage.at[dst], dst_ref=o_all.at[:, my_cols], send_sem=o_send.at[dst],
                                            recv_sem=o_recv.at[me], device_id={"cp": dst},
                                            device_id_type=pl.DeviceIdType.MESH)

    def back_wait(src):
        pltpu.make_async_remote_copy(src_ref=o_stage.at[src], dst_ref=o_all.at[:, aligned(src * head_dim, head_dim)],
                                     send_sem=o_send.at[src], recv_sem=o_recv.at[src], device_id={"cp": src},
                                     device_id_type=pl.DeviceIdType.MESH).wait_recv()

    barrier = pltpu.get_barrier_semaphore()
    for shift in range(1, n_cp):
        pl.semaphore_signal(barrier, inc=1, device_id={"cp": lax.rem(me + shift, n_cp)}, device_id_type=pl.DeviceIdType.MESH)
    load = pltpu.make_async_copy(x_hbm, x_ref, io_sem)
    load.start()
    for which in range(3):
        own_copy(peer(0), 0, which).start()
    load.wait()
    norm_into(x_ref, 0, normed, 0, n_tok)
    pl.semaphore_wait(barrier, n_cp - 1)

    def own_step(step, carry):
        slot = lax.rem(step, 2)
        head = peer(step)

        @pl.when(step + 1 < n_heads)
        def _():
            for which in range(3):
                own_copy(peer(step + 1), 1 - slot, which).start()

        for which in range(3):
            own_copy(head, slot, which).wait()
            for part in range(2):
                stage[head, which, pl.ds(part * half, half), :] = dot_nn(
                    normed[pl.ds(part * half, half), :], w_own[slot, which]).astype(BF16)

        @pl.when(step + 1 < n_heads)
        def _():
            give_copy(head).start()

        return carry

    lax.fori_loop(0, n_heads, own_step, 0)

    def keep_step(idx, carry):
        rows = aligned(idx * 128, 128)
        for which in range(3):
            held[me, which, rows, :] = stage[me, which, rows, :]
        return carry

    lax.fori_loop(0, n_tok // 128, keep_step, 0)
    out_copy(0, 0).start()

    row_id = lax.broadcasted_iota(jnp.int32, (G_ROWS, G_ROWS), 0)
    col_id = lax.broadcasted_iota(jnp.int32, (G_ROWS, G_ROWS), 1)
    per_src = n_tok // G_ROWS

    def block_update(q_src, q_rows, k_src, k_rows, masked):
        scores = dot_nt(held[q_src, 0, q_rows, :], held[k_src, 1, k_rows, :])
        if masked:
            scores = jnp.where(col_id <= row_id, scores, NEG_BIG)
        old_max = run_max[:, :1]
        new_max = jnp.maximum(old_max, jnp.max(scores, axis=-1, keepdims=True))
        probs = jnp.exp2((scores - new_max) * exp_scale)
        rescale = jnp.exp2((old_max - new_max) * exp_scale)
        new_sum = run_sum[:, :1] * rescale + jnp.sum(probs, axis=-1, keepdims=True)
        run_sum[...] = jnp.broadcast_to(new_sum, run_sum.shape)
        run_max[...] = jnp.broadcast_to(new_max, run_max.shape)
        acc[...] = acc[...] * rescale + dot_nn(probs.astype(BF16), held[k_src, 2, k_rows, :])

    def src_step(src, carry):
        @pl.when(src != me)
        def _():
            take_wait(src)

        def row_step(sub, inner):
            q_rows = aligned(sub * G_ROWS, G_ROWS)
            run_max[...] = jnp.full(run_max.shape, NEG_BIG, F32)
            run_sum[...] = jnp.zeros(run_sum.shape, F32)
            acc[...] = jnp.zeros(acc.shape, F32)

            def key_step(key, deep):
                block_update(src, q_rows, key // per_src, aligned(lax.rem(key, per_src) * G_ROWS, G_ROWS), False)
                return deep

            lax.fori_loop(0, src * per_src + sub, key_step, 0)
            block_update(src, q_rows, src, q_rows, True)
            o_stage[src, q_rows, :] = (acc[...] / run_sum[:, :1]).astype(BF16)
            return inner

        lax.fori_loop(0, per_src, row_step, 0)

        @pl.when(src != me)
        def _():
            back_copy(src).start()

        @pl.when(src == me)
        def _():
            o_all[:, my_cols] = o_stage[src]

        return carry

    lax.fori_loop(0, n_cp, src_step, 0)

    def done_step(src, carry):
        @pl.when(src != me)
        def _():
            give_copy(src).wait_send()
            back_copy(src).wait_send()
            back_wait(src)

        return carry

    lax.fori_loop(0, n_cp, done_step, 0)

    def col_step(col, carry):
        slot = lax.rem(col, 2)

        @pl.when(col + 1 < n_cols)
        def _():
            out_copy(col + 1, 1 - slot).start()

        out_copy(col, slot).wait()
        cols = aligned(col * N_COLS, N_COLS)
        for part in range(2):
            rows = pl.ds(part * half, half)
            x_ref[rows, cols] = (x_ref[rows, cols].astype(F32) + dot_nn(o_all[rows, :], w_out[slot])).astype(BF16)
        return carry

    lax.fori_loop(0, n_cols, col_step, 0)
    store = pltpu.make_async_copy(x_ref, out_hbm, io_sem)
    store.start()
    store.wait()


def solution(mesh):
    n_cp = mesh.shape["cp"]

    def device_body(hidden, w_query, w_key, w_value, w_out):
        n_tok, d_model = hidden.shape
        n_layers, _, n_heads, head_dim = w_query.shape
        width = n_heads * head_dim
        dims = (n_tok, d_model, n_heads, head_dim)
        assert n_tok == WINDOW and n_heads == n_cp
        w_heads = [jnp.transpose(w, (0, 2, 1, 3)) for w in (w_query, w_key, w_value)]
        w_flat = w_out.reshape(n_layers, width, d_model)
        any_spec = pl.BlockSpec(memory_space=pl.ANY)
        dma = pltpu.SemaphoreType.DMA
        vmem = pltpu.VMEM
        big = 60 * 1024 * 1024
        flops = 2 * n_tok * d_model * width
        hidden = pl.pallas_call(
            functools.partial(local_layers, n_cp, n_layers - 1, dims),
            out_shape=jax.ShapeDtypeStruct(hidden.shape, hidden.dtype),
            in_specs=[any_spec] * 5, out_specs=any_spec,
            scratch_shapes=[
                vmem((n_tok, d_model), BF16), vmem((n_tok, d_model), BF16), vmem((n_tok, d_model), BF16),
                vmem((n_tok, width), BF16), vmem((2 * n_tok, width), BF16), vmem((2 * n_tok, width), BF16),
                vmem((2, 3, d_model, head_dim), BF16), vmem((2, 2, d_model, head_dim), BF16), vmem((2, width, N_COLS), BF16),
                dma, dma((2, 3)), dma((2, 2)), dma((2,)), dma((2,)), dma((2,)), pltpu.SemaphoreType.REGULAR((2,)),
            ],
            compiler_params=pltpu.CompilerParams(collective_id=0, has_side_effects=True, vmem_limit_bytes=big),
            cost_estimate=pl.CostEstimate(flops=5 * 7 * flops, bytes_accessed=5 * 63 * 2 ** 20, transcendentals=0),
            name="local_layers",
        )(hidden, *w_heads, w_flat)
        order = sorted(range(1, n_cp), key=lambda off: (-min(off, n_cp - off), off)) + [0]
        return pl.pallas_call(
            functools.partial(global_layer, n_cp, n_layers - 1, order, dims),
            out_shape=jax.ShapeDtypeStruct(hidden.shape, hidden.dtype),
            in_specs=[any_spec] * 5, out_specs=any_spec,
            scratch_shapes=[
                vmem((n_tok, d_model), BF16), vmem((n_tok, d_model), BF16),
                vmem((n_heads, 3, n_tok, head_dim), BF16), vmem((n_cp, 3, n_tok, head_dim), BF16),
                vmem((n_cp, n_tok, head_dim), BF16), vmem((n_tok, width), BF16),
                vmem((2, 3, d_model, head_dim), BF16), vmem((2, width, N_COLS), BF16),
                vmem((G_ROWS, 128), F32), vmem((G_ROWS, 128), F32), vmem((G_ROWS, head_dim), F32),
                dma, dma((2, 3)), dma((2,)), dma((n_cp,)), dma((n_cp,)), dma((n_cp,)), dma((n_cp,)),
            ],
            compiler_params=pltpu.CompilerParams(collective_id=1, has_side_effects=True, vmem_limit_bytes=big),
            cost_estimate=pl.CostEstimate(flops=8 * flops, bytes_accessed=63 * 2 ** 20, transcendentals=0),
            name="global_layer",
        )(hidden, *w_heads, w_flat)

    row_spec = P(("dp", "cp"), None)
    return jax.shard_map(device_body, mesh=mesh, in_specs=(row_spec, P(), P(), P(), P()), out_specs=row_spec, check_vma=False)
```

```python
import functools
import math

import jax
import jax.numpy as jnp
from jax import lax
from jax.experimental import pallas as pl
from jax.experimental.pallas import tpu as pltpu
from jax.sharding import PartitionSpec as P

WINDOW = 1024
NORM_EPS = 1e-6
NEG_BIG = -1e30
Q_ROWS = 256
N_COLS = 512
NORM_ROWS = 16
BF16 = jnp.bfloat16
F32 = jnp.float32
NT_DIMS = (((1,), (1,)), ((), ()))


def dot_nt(lhs, rhs):
    return lax.dot_general(lhs, rhs, NT_DIMS, preferred_element_type=F32)


def dot_nn(lhs, rhs):
    return jnp.dot(lhs, rhs, preferred_element_type=F32)


def aligned(start, size):
    return pl.ds(pl.multiple_of(start, size), size)


def norm_into(src_ref, src_row, dst_ref, dst_row, n_rows):
    def body(idx, carry):
        part = src_ref[pl.ds(pl.multiple_of(src_row + idx * NORM_ROWS, NORM_ROWS), NORM_ROWS), :].astype(F32)
        scale = lax.rsqrt(jnp.mean(part * part, axis=-1, keepdims=True) + NORM_EPS)
        dst_ref[pl.ds(pl.multiple_of(dst_row + idx * NORM_ROWS, NORM_ROWS), NORM_ROWS), :] = (part * scale).astype(BF16)
        return carry

    lax.fori_loop(0, n_rows // NORM_ROWS, body, 0, unroll=4)


def local_layers(n_cp, n_run, dims, x_hbm, wq_hbm, wk_hbm, wv_hbm, wo_hbm, out_hbm,
                 x_ref, halo, normed, qo, keys, vals, k_next, v_next, w_own, w_halo, w_out,
                 io_sem, own_sem, halo_sem, out_sem, send_sem, recv_sem, free_sem):
    n_tok, d_model, n_heads, head_dim = dims
    half = n_tok // 2
    n_cols = d_model // N_COLS
    exp_scale = head_dim ** -0.5 * math.log2(math.e)
    me = lax.axis_index("cp")
    right, left = lax.rem(me + 1, n_cp), lax.rem(me + n_cp - 1, n_cp)
    w_in = (wq_hbm, wk_hbm, wv_hbm)

    def own_copy(layer, head, slot, which):
        return pltpu.make_async_copy(w_in[which].at[layer, head], w_own.at[slot, which], own_sem.at[slot, which])

    def halo_copy(layer, head, slot, which):
        return pltpu.make_async_copy(w_in[which + 1].at[layer, head], w_halo.at[slot, which], halo_sem.at[slot, which])

    def out_copy(layer, col, slot):
        return pltpu.make_async_copy(wo_hbm.at[layer, :, aligned(col * N_COLS, N_COLS)], w_out.at[slot], out_sem.at[slot])

    def shift_copy(chunk):
        rows = pl.ds(pl.multiple_of((1 - chunk) * half, half), half)
        return pltpu.make_async_remote_copy(src_ref=x_ref.at[rows], dst_ref=halo.at[rows], send_sem=send_sem.at[chunk],
                                            recv_sem=recv_sem.at[chunk], device_id={"cp": right},
                                            device_id_type=pl.DeviceIdType.MESH)

    barrier = pltpu.get_barrier_semaphore()
    for neighbour in (left, right):
        pl.semaphore_signal(barrier, inc=1, device_id={"cp": neighbour}, device_id_type=pl.DeviceIdType.MESH)
    load = pltpu.make_async_copy(x_hbm, x_ref, io_sem)
    load.start()
    for which in range(3):
        own_copy(0, 0, 0, which).start()
    load.wait()
    pl.semaphore_wait(barrier, 2)
    for chunk in range(2):
        shift_copy(chunk).start()

    row_id = lax.broadcasted_iota(jnp.int32, (Q_ROWS, Q_ROWS), 0)
    col_id = lax.broadcasted_iota(jnp.int32, (Q_ROWS, Q_ROWS), 1)

    n_sub = half // Q_ROWS
    n_blk = WINDOW // Q_ROWS

    def project_halo(slot, which):
        dst = (k_next, v_next)[which]
        dst[...] = dot_nn(normed[pl.ds(0, half), :], w_halo[slot, which]).astype(BF16)

    def soften(scores, q_blk):
        parts = [scores[:, blk * Q_ROWS:(blk + 1) * Q_ROWS] for blk in range(n_blk + 1)]
        parts[0] = jnp.where(col_id > row_id, parts[0], NEG_BIG)
        parts[n_blk] = jnp.where(col_id <= row_id, parts[n_blk], NEG_BIG)
        for blk in range(n_blk):
            parts[blk] = jnp.where((me > 0) | (q_blk + blk >= n_blk), parts[blk], NEG_BIG)
        top = functools.reduce(jnp.maximum, parts)
        top = jnp.max(top, axis=-1, keepdims=True)
        probs = [jnp.exp2((part - top) * exp_scale) for part in parts]
        total = jnp.sum(functools.reduce(jnp.add, probs), axis=-1, keepdims=True)
        return jnp.concatenate([prob.astype(BF16) for prob in probs], axis=1), total

    def attend(chunk, cols, side_k, side_v):
        blks = [(1 - chunk) * n_sub + sub for sub in range(n_sub)]
        q_rows = [aligned(blk * Q_ROWS, Q_ROWS) for blk in blks]
        k_rows = [pl.ds(pl.multiple_of(blk * Q_ROWS, Q_ROWS), WINDOW + Q_ROWS) for blk in blks]
        scores = [dot_nt(qo[q_rows[sub], cols], keys[k_rows[sub], cols]) for sub in range(n_sub)]
        side_k()
        soft = [soften(scores[sub], blks[sub]) for sub in range(n_sub)]
        side_v()
        outs = [dot_nn(soft[sub][0], vals[k_rows[sub], cols]) / soft[sub][1] for sub in range(n_sub)]
        for sub in range(n_sub):
            qo[q_rows[sub], cols] = outs[sub].astype(BF16)

    def layer_step(layer, carry):
        norm_into(x_ref, 0, normed, 0, n_tok)
        for head in range(2):
            for which in range(2):
                halo_copy(layer, head, head, which).start()

        def own_step(head, inner):
            slot = lax.rem(head, 2)

            @pl.when(head + 1 < n_heads)
            def _():
                for which in range(3):
                    own_copy(layer, head + 1, 1 - slot, which).start()

            cols = aligned(head * head_dim, head_dim)
            for which, (dst, base) in enumerate(((qo, 0), (keys, n_tok), (vals, n_tok))):
                own_copy(layer, head, slot, which).wait()
                for part in range(2):
                    dst[pl.ds(base + part * half, half), cols] = dot_nn(
                        normed[pl.ds(part * half, half), :], w_own[slot, which]).astype(BF16)
            return inner

        lax.fori_loop(0, n_heads, own_step, 0)

        def chunk_step(chunk, inner):
            row0 = pl.multiple_of((1 - chunk) * half, half)
            rows = pl.ds(row0, half)
            shift_copy(chunk).wait_recv()
            norm_into(halo, row0, normed, 0, half)

            @pl.when(layer + 1 < n_run)
            def _():
                pl.semaphore_signal(free_sem.at[chunk], inc=1, device_id={"cp": left}, device_id_type=pl.DeviceIdType.MESH)

            out_copy(layer, 0, 0).start()

            def keep(cols):
                keys[rows, cols] = k_next[...]
                vals[rows, cols] = v_next[...]

            for which in range(2):
                halo_copy(layer, 0, 0, which).wait()
                project_halo(0, which)

            def head_step(head, deep):
                slot = lax.rem(head, 2)

                @pl.when(head + 2 < n_heads)
                def _():
                    for which in range(2):
                        halo_copy(layer, head + 2, slot, which).start()

                @pl.when((head + 2 == n_heads) & (chunk == 0))
                def _():
                    for which in range(2):
                        halo_copy(layer, 0, slot, which).start()

                @pl.when((head + 2 == n_heads) & (chunk == 1) & (layer + 1 < n_run))
                def _():
                    for which in range(3):
                        own_copy(layer + 1, 0, 0, which).start()

                for which in range(2):
                    halo_copy(layer, head + 1, 1 - slot, which).wait()
                cols = aligned(head * head_dim, head_dim)
                keep(cols)
                attend(chunk, cols, lambda: project_halo(1 - slot, 0), lambda: project_halo(1 - slot, 1))
                return deep

            lax.fori_loop(0, n_heads - 1, head_step, 0)

            @pl.when(chunk == 0)
            def _():
                for which in range(2):
                    halo_copy(layer, 1, 1, which).start()

            last = pl.ds((n_heads - 1) * head_dim, head_dim)
            keep(last)
            attend(chunk, last, lambda: None, lambda: None)
            shift_copy(chunk).wait_send()

            def col_step(col, deep):
                slot = lax.rem(col, 2)

                @pl.when(col + 1 < n_cols)
                def _():
                    out_copy(layer, col + 1, 1 - slot).start()

                out_copy(layer, col, slot).wait()
                cols = aligned(col * N_COLS, N_COLS)
                x_ref[rows, cols] = (x_ref[rows, cols].astype(F32) + dot_nn(qo[rows, :], w_out[slot])).astype(BF16)
                return deep

            lax.fori_loop(0, n_cols, col_step, 0)

            @pl.when(layer + 1 < n_run)
            def _():
                pl.semaphore_wait(free_sem.at[chunk], 1)
                shift_copy(chunk).start()

            return inner

        lax.fori_loop(0, 2, chunk_step, 0)
        return carry

    lax.fori_loop(0, n_run, layer_step, 0)
    store = pltpu.make_async_copy(x_ref, out_hbm, io_sem)
    store.start()
    store.wait()


def global_layer(n_cp, layer, dims, x_hbm, wq_hbm, wk_hbm, wv_hbm, wo_hbm, out_hbm,
                 x_ref, stage, held, relay, o_stage, o_all, w_own, w_out, *rest):
    n_tok, d_model, n_heads, head_dim = dims
    half = n_tok // 2
    n_cols = d_model // N_COLS
    exp_scale = head_dim ** -0.5 * math.log2(math.e)
    n_grp = n_tok // Q_ROWS
    run_max, run_sum, acc = rest[:n_grp], rest[n_grp:2 * n_grp], rest[2 * n_grp:3 * n_grp]
    io_sem, own_sem, out_sem, send_sem, recv_sem, o_send, o_recv, relay_send, relay_recv = rest[3 * n_grp:]
    me = lax.axis_index("cp")
    w_in = (wq_hbm, wk_hbm, wv_hbm)
    mate = me + 1 - 2 * lax.rem(me, 2)
    far, back = n_cp // 2, n_cp - 2
    via = lax.rem(me + back, n_cp)
    relay_dst = lax.rem(mate + far, n_cp)
    relay_src = lax.rem(me + 2, n_cp)
    relay_end = lax.rem(mate + back, n_cp)
    peers = [relay_dst, lax.rem(me + far, n_cp), lax.rem(me + 2, n_cp), lax.rem(me + back, n_cp),
             lax.rem(mate + 2, n_cp), lax.rem(mate + back, n_cp), mate, me]

    def peer(step):
        head = me
        for idx, other in enumerate(peers):
            head = jnp.where(step == idx, other, head)
        return head

    def own_copy(head, slot, which):
        return pltpu.make_async_copy(w_in[which].at[layer, head], w_own.at[slot, which], own_sem.at[slot, which])

    def out_copy(col, slot):
        return pltpu.make_async_copy(wo_hbm.at[layer, :, aligned(col * N_COLS, N_COLS)], w_out.at[slot], out_sem.at[slot])

    def give_copy(dst):
        return pltpu.make_async_remote_copy(src_ref=stage.at[dst], dst_ref=held.at[me], send_sem=send_sem.at[dst],
                                            recv_sem=recv_sem.at[me], device_id={"cp": dst},
                                            device_id_type=pl.DeviceIdType.MESH)

    def relay_copy():
        return pltpu.make_async_remote_copy(src_ref=stage.at[relay_dst], dst_ref=relay, send_sem=send_sem.at[relay_dst],
                                            recv_sem=relay_recv, device_id={"cp": via},
                                            device_id_type=pl.DeviceIdType.MESH)

    def forward_copy():
        return pltpu.make_async_remote_copy(src_ref=relay, dst_ref=held.at[relay_src], send_sem=relay_send,
                                            recv_sem=recv_sem.at[relay_src], device_id={"cp": relay_end},
                                            device_id_type=pl.DeviceIdType.MESH)

    def take_wait(src):
        pltpu.make_async_remote_copy(src_ref=held.at[src], dst_ref=held.at[src], send_sem=send_sem.at[src],
                                     recv_sem=recv_sem.at[src], device_id={"cp": src},
                                     device_id_type=pl.DeviceIdType.MESH).wait_recv()

    my_cols = aligned(me * head_dim, head_dim)

    def back_copy(dst):
        return pltpu.make_async_remote_copy(src_ref=o_stage.at[dst], dst_ref=o_all.at[:, my_cols], send_sem=o_send.at[dst],
                                            recv_sem=o_recv.at[me], device_id={"cp": dst},
                                            device_id_type=pl.DeviceIdType.MESH)

    def back_wait(src):
        pltpu.make_async_remote_copy(src_ref=o_stage.at[src], dst_ref=o_all.at[:, aligned(src * head_dim, head_dim)],
                                     send_sem=o_send.at[src], recv_sem=o_recv.at[src], device_id={"cp": src},
                                     device_id_type=pl.DeviceIdType.MESH).wait_recv()

    barrier = pltpu.get_barrier_semaphore()
    for shift in range(1, n_cp):
        pl.semaphore_signal(barrier, inc=1, device_id={"cp": lax.rem(me + shift, n_cp)}, device_id_type=pl.DeviceIdType.MESH)
    load = pltpu.make_async_copy(x_hbm, x_ref, io_sem)
    load.start()
    for which in range(3):
        own_copy(peer(0), 0, which).start()
    load.wait()
    norm_into(x_ref, 0, x_ref, 0, n_tok)
    pl.semaphore_wait(barrier, n_cp - 1)

    def own_step(step, carry):
        slot = lax.rem(step, 2)
        head = peer(step)

        @pl.when(step + 1 < n_heads)
        def _():
            for which in range(3):
                own_copy(peer(step + 1), 1 - slot, which).start()

        for which in range(3):
            own_copy(head, slot, which).wait()
            for part in range(2):
                stage[head, which, pl.ds(part * half, half), :] = dot_nn(
                    x_ref[pl.ds(part * half, half), :], w_own[slot, which]).astype(BF16)

        @pl.when(step == 0)
        def _():
            relay_copy().start()

        @pl.when((step > 0) & (step + 1 < n_heads))
        def _():
            give_copy(head).start()

        return carry

    lax.fori_loop(0, n_heads, own_step, 0)
    load.start()
    relay_copy().wait_recv()
    forward_copy().start()

    def keep_step(idx, carry):
        rows = aligned(idx * 128, 128)
        for which in range(3):
            held[me, which, rows, :] = stage[me, which, rows, :]
        return carry

    lax.fori_loop(0, n_tok // 128, keep_step, 0)
    out_copy(0, 0).start()

    row_id = lax.broadcasted_iota(jnp.int32, (Q_ROWS, Q_ROWS), 0)
    col_id = lax.broadcasted_iota(jnp.int32, (Q_ROWS, Q_ROWS), 1)
    grp_rows = [pl.ds(grp * Q_ROWS, Q_ROWS) for grp in range(n_grp)]

    def score(q_src, k_src, grp, n_key):
        return dot_nt(held[q_src, 0, grp_rows[grp], :], held[k_src, 1, pl.ds(0, n_key), :])

    def update(grp, scores, k_src, n_key, first):
        new_max = jnp.max(scores, axis=-1, keepdims=True)
        if not first:
            old_max = run_max[grp][:, :1]
            new_max = jnp.maximum(old_max, new_max)
        probs = jnp.exp2((scores - new_max) * exp_scale)
        new_sum = jnp.sum(probs, axis=-1, keepdims=True)
        if not first:
            rescale = jnp.exp2((old_max - new_max) * exp_scale)
            new_sum = run_sum[grp][:, :1] * rescale + new_sum
        run_sum[grp][...] = jnp.broadcast_to(new_sum, run_sum[grp].shape)
        run_max[grp][...] = jnp.broadcast_to(new_max, run_max[grp].shape)
        new_acc = dot_nn(probs.astype(BF16), held[k_src, 2, pl.ds(0, n_key), :])
        acc[grp][...] = new_acc if first else acc[grp][...] * rescale + new_acc

    def src_step(src, carry):
        @pl.when(src != me)
        def _():
            take_wait(src)

        scores = []
        for grp in range(n_grp):
            full = score(src, src, grp, (grp + 1) * Q_ROWS)
            diag = jnp.where(col_id <= row_id, full[:, grp * Q_ROWS:], NEG_BIG)
            scores.append(jnp.concatenate([full[:, :grp * Q_ROWS], diag], axis=1) if grp else diag)
        for grp in range(n_grp):
            update(grp, scores[grp], src, (grp + 1) * Q_ROWS, True)

        def key_step(k_src, inner):
            ready = [score(src, k_src, 0, n_tok)]
            for grp in range(n_grp):
                if grp + 1 < n_grp:
                    ready.append(score(src, k_src, grp + 1, n_tok))
                update(grp, ready[grp], k_src, n_tok, False)
            return inner

        lax.fori_loop(0, src, key_step, 0)
        for grp in range(n_grp):
            o_stage[src, grp_rows[grp], :] = (acc[grp][...] / run_sum[grp][:, :1]).astype(BF16)

        @pl.when(src != me)
        def _():
            back_copy(src).start()

        @pl.when(src == me)
        def _():
            o_all[:, my_cols] = o_stage[src]

        return carry

    lax.fori_loop(0, n_cp, src_step, 0)

    forward_copy().wait_send()

    def done_step(src, carry):
        @pl.when(src != me)
        def _():
            @pl.when(src == relay_dst)
            def _():
                relay_copy().wait_send()

            @pl.when(src != relay_dst)
            def _():
                give_copy(src).wait_send()

            back_copy(src).wait_send()
            back_wait(src)

        return carry

    lax.fori_loop(0, n_cp, done_step, 0)

    load.wait()

    def col_step(col, carry):
        slot = lax.rem(col, 2)

        @pl.when(col + 1 < n_cols)
        def _():
            out_copy(col + 1, 1 - slot).start()

        out_copy(col, slot).wait()
        cols = aligned(col * N_COLS, N_COLS)
        for part in range(2):
            rows = pl.ds(part * half, half)
            x_ref[rows, cols] = (x_ref[rows, cols].astype(F32) + dot_nn(o_all[rows, :], w_out[slot])).astype(BF16)
        return carry

    lax.fori_loop(0, n_cols, col_step, 0)
    store = pltpu.make_async_copy(x_ref, out_hbm, io_sem)
    store.start()
    store.wait()


def solution(mesh):
    n_cp = mesh.shape["cp"]

    def device_body(hidden, w_query, w_key, w_value, w_out):
        n_tok, d_model = hidden.shape
        n_layers, _, n_heads, head_dim = w_query.shape
        width = n_heads * head_dim
        dims = (n_tok, d_model, n_heads, head_dim)
        assert n_tok == WINDOW and n_heads == n_cp
        w_heads = [jnp.transpose(w, (0, 2, 1, 3)) for w in (w_query, w_key, w_value)]
        w_flat = w_out.reshape(n_layers, width, d_model)
        any_spec = pl.BlockSpec(memory_space=pl.ANY)
        dma = pltpu.SemaphoreType.DMA
        vmem = pltpu.VMEM
        big = 60 * 1024 * 1024
        flops = 2 * n_tok * d_model * width
        hidden = pl.pallas_call(
            functools.partial(local_layers, n_cp, n_layers - 1, dims),
            out_shape=jax.ShapeDtypeStruct(hidden.shape, hidden.dtype),
            in_specs=[any_spec] * 5, out_specs=any_spec,
            scratch_shapes=[
                vmem((n_tok, d_model), BF16), vmem((n_tok, d_model), BF16), vmem((n_tok, d_model), BF16),
                vmem((n_tok, width), BF16), vmem((2 * n_tok, width), BF16), vmem((2 * n_tok, width), BF16),
                vmem((n_tok // 2, head_dim), BF16), vmem((n_tok // 2, head_dim), BF16),
                vmem((2, 3, d_model, head_dim), BF16), vmem((2, 2, d_model, head_dim), BF16), vmem((2, width, N_COLS), BF16),
                dma, dma((2, 3)), dma((2, 2)), dma((2,)), dma((2,)), dma((2,)), pltpu.SemaphoreType.REGULAR((2,)),
            ],
            compiler_params=pltpu.CompilerParams(collective_id=0, has_side_effects=True, vmem_limit_bytes=big),
            cost_estimate=pl.CostEstimate(flops=5 * 7 * flops, bytes_accessed=5 * 63 * 2 ** 20, transcendentals=0),
            name="local_layers",
        )(hidden, *w_heads, w_flat)
        n_grp = n_tok // Q_ROWS
        return pl.pallas_call(
            functools.partial(global_layer, n_cp, n_layers - 1, dims),
            out_shape=jax.ShapeDtypeStruct(hidden.shape, hidden.dtype),
            in_specs=[any_spec] * 5, out_specs=any_spec,
            scratch_shapes=[
                vmem((n_tok, d_model), BF16),
                vmem((n_heads, 3, n_tok, head_dim), BF16), vmem((n_cp, 3, n_tok, head_dim), BF16),
                vmem((3, n_tok, head_dim), BF16), vmem((n_cp, n_tok, head_dim), BF16), vmem((n_tok, width), BF16),
                vmem((2, 3, d_model, head_dim), BF16), vmem((2, width, N_COLS), BF16),
                *[vmem((Q_ROWS, 128), F32)] * (2 * n_grp), *[vmem((Q_ROWS, head_dim), F32)] * n_grp,
                dma, dma((2, 3)), dma((2,)), dma((n_cp,)), dma((n_cp,)), dma((n_cp,)), dma((n_cp,)), dma, dma,
            ],
            compiler_params=pltpu.CompilerParams(collective_id=1, has_side_effects=True, vmem_limit_bytes=big),
            cost_estimate=pl.CostEstimate(flops=8 * flops, bytes_accessed=63 * 2 ** 20, transcendentals=0),
            name="global_layer",
        )(hidden, *w_heads, w_flat)

    row_spec = P(("dp", "cp"), None)
    return jax.shard_map(device_body, mesh=mesh, in_specs=(row_spec, P(), P(), P(), P()), out_specs=row_spec, check_vma=False)
```

```python
import functools
import math

import jax
import jax.numpy as jnp
from jax import lax
from jax.experimental import pallas as pl
from jax.experimental.pallas import tpu as pltpu
from jax.sharding import PartitionSpec as P

WINDOW = 1024
NORM_EPS = 1e-6
NEG_BIG = -1e30
Q_ROWS = 256
N_COLS = 512
NORM_ROWS = 16
BF16 = jnp.bfloat16
F32 = jnp.float32
NT_DIMS = (((1,), (1,)), ((), ()))


def dot_nt(lhs, rhs):
    return lax.dot_general(lhs, rhs, NT_DIMS, preferred_element_type=F32)


def dot_nn(lhs, rhs):
    return jnp.dot(lhs, rhs, preferred_element_type=F32)


def aligned(start, size):
    return pl.ds(pl.multiple_of(start, size), size)


def norm_into(src_ref, src_row, dst_ref, dst_row, n_rows):
    def body(idx, carry):
        part = src_ref[pl.ds(pl.multiple_of(src_row + idx * NORM_ROWS, NORM_ROWS), NORM_ROWS), :].astype(F32)
        scale = lax.rsqrt(jnp.mean(part * part, axis=-1, keepdims=True) + NORM_EPS)
        dst_ref[pl.ds(pl.multiple_of(dst_row + idx * NORM_ROWS, NORM_ROWS), NORM_ROWS), :] = (part * scale).astype(BF16)
        return carry

    lax.fori_loop(0, n_rows // NORM_ROWS, body, 0, unroll=4)


def local_layers(n_cp, n_run, dims, x_hbm, wq_hbm, wk_hbm, wv_hbm, wo_hbm, out_hbm,
                 x_ref, halo, normed, qo, keys, vals, k_next, v_next, w_own, w_halo, w_out,
                 io_sem, own_sem, halo_sem, out_sem, send_sem, recv_sem, free_sem):
    n_tok, d_model, n_heads, head_dim = dims
    half = n_tok // 2
    n_cols = d_model // N_COLS
    exp_scale = head_dim ** -0.5 * math.log2(math.e)
    me = lax.axis_index("cp")
    right, left = lax.rem(me + 1, n_cp), lax.rem(me + n_cp - 1, n_cp)
    w_in = (wq_hbm, wk_hbm, wv_hbm)

    def own_copy(layer, head, slot, which):
        return pltpu.make_async_copy(w_in[which].at[layer, head], w_own.at[slot, which], own_sem.at[slot, which])

    def halo_copy(layer, head, slot, which):
        return pltpu.make_async_copy(w_in[which + 1].at[layer, head], w_halo.at[slot, which], halo_sem.at[slot, which])

    def out_copy(layer, col, slot):
        return pltpu.make_async_copy(wo_hbm.at[layer, :, aligned(col * N_COLS, N_COLS)], w_out.at[slot], out_sem.at[slot])

    def shift_copy(chunk):
        rows = pl.ds(pl.multiple_of((1 - chunk) * half, half), half)
        return pltpu.make_async_remote_copy(src_ref=x_ref.at[rows], dst_ref=halo.at[rows], send_sem=send_sem.at[chunk],
                                            recv_sem=recv_sem.at[chunk], device_id={"cp": right},
                                            device_id_type=pl.DeviceIdType.MESH)

    barrier = pltpu.get_barrier_semaphore()
    for neighbour in (left, right):
        pl.semaphore_signal(barrier, inc=1, device_id={"cp": neighbour}, device_id_type=pl.DeviceIdType.MESH)
    load = pltpu.make_async_copy(x_hbm, x_ref, io_sem)
    load.start()
    for which in range(3):
        own_copy(0, 0, 0, which).start()
    load.wait()
    pl.semaphore_wait(barrier, 2)
    for chunk in range(2):
        shift_copy(chunk).start()

    row_id = lax.broadcasted_iota(jnp.int32, (Q_ROWS, Q_ROWS), 0)
    col_id = lax.broadcasted_iota(jnp.int32, (Q_ROWS, Q_ROWS), 1)

    n_sub = half // Q_ROWS
    n_blk = WINDOW // Q_ROWS

    def project_halo(slot, which):
        dst = (k_next, v_next)[which]
        dst[...] = dot_nn(normed[pl.ds(0, half), :], w_halo[slot, which]).astype(BF16)

    def soften(scores, q_blk):
        parts = [scores[:, blk * Q_ROWS:(blk + 1) * Q_ROWS] for blk in range(n_blk + 1)]
        parts[0] = jnp.where(col_id > row_id, parts[0], NEG_BIG)
        parts[n_blk] = jnp.where(col_id <= row_id, parts[n_blk], NEG_BIG)
        for blk in range(n_blk):
            parts[blk] = jnp.where((me > 0) | (q_blk + blk >= n_blk), parts[blk], NEG_BIG)
        top = functools.reduce(jnp.maximum, parts)
        top = jnp.max(top, axis=-1, keepdims=True)
        probs = [jnp.exp2((part - top) * exp_scale) for part in parts]
        total = jnp.sum(functools.reduce(jnp.add, probs), axis=-1, keepdims=True)
        return jnp.concatenate([prob.astype(BF16) for prob in probs], axis=1), total

    def attend(chunk, cols, side_k, side_v):
        blks = [(1 - chunk) * n_sub + sub for sub in range(n_sub)]
        q_rows = [aligned(blk * Q_ROWS, Q_ROWS) for blk in blks]
        k_rows = [pl.ds(pl.multiple_of(blk * Q_ROWS, Q_ROWS), WINDOW + Q_ROWS) for blk in blks]
        scores = [dot_nt(qo[q_rows[sub], cols], keys[k_rows[sub], cols]) for sub in range(n_sub)]
        side_k()
        soft = [soften(scores[sub], blks[sub]) for sub in range(n_sub)]
        side_v()
        outs = [dot_nn(soft[sub][0], vals[k_rows[sub], cols]) / soft[sub][1] for sub in range(n_sub)]
        for sub in range(n_sub):
            qo[q_rows[sub], cols] = outs[sub].astype(BF16)

    def layer_step(layer, carry):
        norm_into(x_ref, 0, normed, 0, n_tok)
        for head in range(2):
            for which in range(2):
                halo_copy(layer, head, head, which).start()

        def own_step(head, inner):
            slot = lax.rem(head, 2)

            @pl.when(head + 1 < n_heads)
            def _():
                for which in range(3):
                    own_copy(layer, head + 1, 1 - slot, which).start()

            cols = aligned(head * head_dim, head_dim)
            for which, (dst, base) in enumerate(((qo, 0), (keys, n_tok), (vals, n_tok))):
                own_copy(layer, head, slot, which).wait()
                for part in range(2):
                    dst[pl.ds(base + part * half, half), cols] = dot_nn(
                        normed[pl.ds(part * half, half), :], w_own[slot, which]).astype(BF16)
            return inner

        lax.fori_loop(0, n_heads, own_step, 0)

        def chunk_step(chunk, inner):
            row0 = pl.multiple_of((1 - chunk) * half, half)
            rows = pl.ds(row0, half)
            shift_copy(chunk).wait_recv()
            norm_into(halo, row0, normed, 0, half)

            @pl.when(layer + 1 < n_run)
            def _():
                pl.semaphore_signal(free_sem.at[chunk], inc=1, device_id={"cp": left}, device_id_type=pl.DeviceIdType.MESH)

            out_copy(layer, 0, 0).start()

            def keep(cols):
                keys[rows, cols] = k_next[...]
                vals[rows, cols] = v_next[...]

            for which in range(2):
                halo_copy(layer, 0, 0, which).wait()
                project_halo(0, which)

            def head_step(head, deep):
                slot = lax.rem(head, 2)

                @pl.when(head + 2 < n_heads)
                def _():
                    for which in range(2):
                        halo_copy(layer, head + 2, slot, which).start()

                @pl.when((head + 2 == n_heads) & (chunk == 0))
                def _():
                    for which in range(2):
                        halo_copy(layer, 0, slot, which).start()

                @pl.when((head + 2 == n_heads) & (chunk == 1) & (layer + 1 < n_run))
                def _():
                    for which in range(3):
                        own_copy(layer + 1, 0, 0, which).start()

                for which in range(2):
                    halo_copy(layer, head + 1, 1 - slot, which).wait()
                cols = aligned(head * head_dim, head_dim)
                keep(cols)
                attend(chunk, cols, lambda: project_halo(1 - slot, 0), lambda: project_halo(1 - slot, 1))
                return deep

            lax.fori_loop(0, n_heads - 1, head_step, 0)

            @pl.when(chunk == 0)
            def _():
                for which in range(2):
                    halo_copy(layer, 1, 1, which).start()

            last = pl.ds((n_heads - 1) * head_dim, head_dim)
            keep(last)
            attend(chunk, last, lambda: None, lambda: None)
            shift_copy(chunk).wait_send()

            def col_step(col, deep):
                slot = lax.rem(col, 2)

                @pl.when(col + 1 < n_cols)
                def _():
                    out_copy(layer, col + 1, 1 - slot).start()

                out_copy(layer, col, slot).wait()
                cols = aligned(col * N_COLS, N_COLS)
                x_ref[rows, cols] = (x_ref[rows, cols].astype(F32) + dot_nn(qo[rows, :], w_out[slot])).astype(BF16)
                return deep

            lax.fori_loop(0, n_cols, col_step, 0)

            @pl.when(layer + 1 < n_run)
            def _():
                pl.semaphore_wait(free_sem.at[chunk], 1)
                shift_copy(chunk).start()

            return inner

        lax.fori_loop(0, 2, chunk_step, 0)
        return carry

    lax.fori_loop(0, n_run, layer_step, 0)
    store = pltpu.make_async_copy(x_ref, out_hbm, io_sem)
    store.start()
    store.wait()


def global_layer(n_cp, layer, dims, x_hbm, wq_hbm, wk_hbm, wv_hbm, wo_hbm, out_hbm,
                 x_ref, stage, held, o_stage, o_all, w_own, w_out, *rest):
    n_tok, d_model, n_heads, head_dim = dims
    half = n_tok // 2
    n_cols = d_model // N_COLS
    exp_scale = head_dim ** -0.5 * math.log2(math.e)
    n_grp = n_tok // Q_ROWS
    run_max, run_sum, acc = rest[:n_grp], rest[n_grp:2 * n_grp], rest[2 * n_grp:3 * n_grp]
    io_sem, own_sem, out_sem, send_sem, recv_sem, o_send, o_recv = rest[3 * n_grp:]
    me = lax.axis_index("cp")
    w_in = (wq_hbm, wk_hbm, wv_hbm)
    mate = me + 1 - 2 * lax.rem(me, 2)
    far, back = n_cp // 2, n_cp - 2
    peers = [lax.rem(mate + far, n_cp), lax.rem(me + far, n_cp), lax.rem(me + 2, n_cp), lax.rem(me + back, n_cp),
             lax.rem(mate + 2, n_cp), lax.rem(mate + back, n_cp), mate, me]

    def peer(step):
        head = me
        for idx, other in enumerate(peers):
            head = jnp.where(step == idx, other, head)
        return head

    def own_copy(head, slot, which):
        return pltpu.make_async_copy(w_in[which].at[layer, head], w_own.at[slot, which], own_sem.at[slot, which])

    def out_copy(col, slot):
        return pltpu.make_async_copy(wo_hbm.at[layer, :, aligned(col * N_COLS, N_COLS)], w_out.at[slot], out_sem.at[slot])

    def give_copy(dst):
        return pltpu.make_async_remote_copy(src_ref=stage.at[dst], dst_ref=held.at[me], send_sem=send_sem.at[dst],
                                            recv_sem=recv_sem.at[me], device_id={"cp": dst},
                                            device_id_type=pl.DeviceIdType.MESH)

    def take_wait(src):
        pltpu.make_async_remote_copy(src_ref=held.at[src], dst_ref=held.at[src], send_sem=send_sem.at[src],
                                     recv_sem=recv_sem.at[src], device_id={"cp": src},
                                     device_id_type=pl.DeviceIdType.MESH).wait_recv()

    my_cols = aligned(me * head_dim, head_dim)

    def back_copy(dst):
        return pltpu.make_async_remote_copy(src_ref=o_stage.at[dst], dst_ref=o_all.at[:, my_cols], send_sem=o_send.at[dst],
                                            recv_sem=o_recv.at[me], device_id={"cp": dst},
                                            device_id_type=pl.DeviceIdType.MESH)

    def back_wait(src):
        pltpu.make_async_remote_copy(src_ref=o_stage.at[src], dst_ref=o_all.at[:, aligned(src * head_dim, head_dim)],
                                     send_sem=o_send.at[src], recv_sem=o_recv.at[src], device_id={"cp": src},
                                     device_id_type=pl.DeviceIdType.MESH).wait_recv()

    barrier = pltpu.get_barrier_semaphore()
    for shift in range(1, n_cp):
        pl.semaphore_signal(barrier, inc=1, device_id={"cp": lax.rem(me + shift, n_cp)}, device_id_type=pl.DeviceIdType.MESH)
    load = pltpu.make_async_copy(x_hbm, x_ref, io_sem)
    load.start()
    for which in range(3):
        own_copy(peer(0), 0, which).start()
    load.wait()
    norm_into(x_ref, 0, x_ref, 0, n_tok)
    pl.semaphore_wait(barrier, n_cp - 1)

    def own_step(step, carry):
        slot = lax.rem(step, 2)
        head = peer(step)

        @pl.when(step + 1 < n_heads)
        def _():
            for which in range(3):
                own_copy(peer(step + 1), 1 - slot, which).start()

        for which in range(3):
            own_copy(head, slot, which).wait()
            for part in range(2):
                stage[head, which, pl.ds(part * half, half), :] = dot_nn(
                    x_ref[pl.ds(part * half, half), :], w_own[slot, which]).astype(BF16)

        @pl.when(step + 1 < n_heads)
        def _():
            give_copy(head).start()

        return carry

    lax.fori_loop(0, n_heads, own_step, 0)
    load.start()

    def keep_step(idx, carry):
        rows = aligned(idx * 128, 128)
        for which in range(3):
            held[me, which, rows, :] = stage[me, which, rows, :]
        return carry

    lax.fori_loop(0, n_tok // 128, keep_step, 0)
    out_copy(0, 0).start()

    row_id = lax.broadcasted_iota(jnp.int32, (Q_ROWS, Q_ROWS), 0)
    col_id = lax.broadcasted_iota(jnp.int32, (Q_ROWS, Q_ROWS), 1)
    grp_rows = [pl.ds(grp * Q_ROWS, Q_ROWS) for grp in range(n_grp)]

    def score(q_src, k_src, grp, n_key):
        return dot_nt(held[q_src, 0, grp_rows[grp], :], held[k_src, 1, pl.ds(0, n_key), :])

    def update(grp, scores, k_src, n_key, first):
        new_max = jnp.max(scores, axis=-1, keepdims=True)
        if not first:
            old_max = run_max[grp][:, :1]
            new_max = jnp.maximum(old_max, new_max)
        probs = jnp.exp2((scores - new_max) * exp_scale)
        new_sum = jnp.sum(probs, axis=-1, keepdims=True)
        if not first:
            rescale = jnp.exp2((old_max - new_max) * exp_scale)
            new_sum = run_sum[grp][:, :1] * rescale + new_sum
        run_sum[grp][...] = jnp.broadcast_to(new_sum, run_sum[grp].shape)
        run_max[grp][...] = jnp.broadcast_to(new_max, run_max[grp].shape)
        new_acc = dot_nn(probs.astype(BF16), held[k_src, 2, pl.ds(0, n_key), :])
        acc[grp][...] = new_acc if first else acc[grp][...] * rescale + new_acc

    def src_step(src, carry):
        @pl.when(src != me)
        def _():
            take_wait(src)

        scores = []
        for grp in range(n_grp):
            full = score(src, src, grp, (grp + 1) * Q_ROWS)
            diag = jnp.where(col_id <= row_id, full[:, grp * Q_ROWS:], NEG_BIG)
            scores.append(jnp.concatenate([full[:, :grp * Q_ROWS], diag], axis=1) if grp else diag)
        for grp in range(n_grp):
            update(grp, scores[grp], src, (grp + 1) * Q_ROWS, True)

        def key_step(k_src, inner):
            ready = [score(src, k_src, 0, n_tok)]
            for grp in range(n_grp):
                if grp + 1 < n_grp:
                    ready.append(score(src, k_src, grp + 1, n_tok))
                update(grp, ready[grp], k_src, n_tok, False)
            return inner

        lax.fori_loop(0, src, key_step, 0)
        for grp in range(n_grp):
            o_stage[src, grp_rows[grp], :] = (acc[grp][...] / run_sum[grp][:, :1]).astype(BF16)

        @pl.when(src != me)
        def _():
            back_copy(src).start()

        @pl.when(src == me)
        def _():
            o_all[:, my_cols] = o_stage[src]

        return carry

    lax.fori_loop(0, n_cp, src_step, 0)


    def done_step(src, carry):
        @pl.when(src != me)
        def _():
            give_copy(src).wait_send()

            back_copy(src).wait_send()
            back_wait(src)

        return carry

    lax.fori_loop(0, n_cp, done_step, 0)

    load.wait()

    def col_step(col, carry):
        slot = lax.rem(col, 2)

        @pl.when(col + 1 < n_cols)
        def _():
            out_copy(col + 1, 1 - slot).start()

        out_copy(col, slot).wait()
        cols = aligned(col * N_COLS, N_COLS)
        for part in range(2):
            rows = pl.ds(part * half, half)
            x_ref[rows, cols] = (x_ref[rows, cols].astype(F32) + dot_nn(o_all[rows, :], w_out[slot])).astype(BF16)
        return carry

    lax.fori_loop(0, n_cols, col_step, 0)
    store = pltpu.make_async_copy(x_ref, out_hbm, io_sem)
    store.start()
    store.wait()


def solution(mesh):
    n_cp = mesh.shape["cp"]

    def device_body(hidden, w_query, w_key, w_value, w_out):
        n_tok, d_model = hidden.shape
        n_layers, _, n_heads, head_dim = w_query.shape
        width = n_heads * head_dim
        dims = (n_tok, d_model, n_heads, head_dim)
        assert n_tok == WINDOW and n_heads == n_cp
        w_heads = [jnp.transpose(w, (0, 2, 1, 3)) for w in (w_query, w_key, w_value)]
        w_flat = w_out.reshape(n_layers, width, d_model)
        any_spec = pl.BlockSpec(memory_space=pl.ANY)
        dma = pltpu.SemaphoreType.DMA
        vmem = pltpu.VMEM
        big = 60 * 1024 * 1024
        flops = 2 * n_tok * d_model * width
        hidden = pl.pallas_call(
            functools.partial(local_layers, n_cp, n_layers - 1, dims),
            out_shape=jax.ShapeDtypeStruct(hidden.shape, hidden.dtype),
            in_specs=[any_spec] * 5, out_specs=any_spec,
            scratch_shapes=[
                vmem((n_tok, d_model), BF16), vmem((n_tok, d_model), BF16), vmem((n_tok, d_model), BF16),
                vmem((n_tok, width), BF16), vmem((2 * n_tok, width), BF16), vmem((2 * n_tok, width), BF16),
                vmem((n_tok // 2, head_dim), BF16), vmem((n_tok // 2, head_dim), BF16),
                vmem((2, 3, d_model, head_dim), BF16), vmem((2, 2, d_model, head_dim), BF16), vmem((2, width, N_COLS), BF16),
                dma, dma((2, 3)), dma((2, 2)), dma((2,)), dma((2,)), dma((2,)), pltpu.SemaphoreType.REGULAR((2,)),
            ],
            compiler_params=pltpu.CompilerParams(collective_id=0, has_side_effects=True, vmem_limit_bytes=big),
            cost_estimate=pl.CostEstimate(flops=5 * 7 * flops, bytes_accessed=5 * 63 * 2 ** 20, transcendentals=0),
            name="local_layers",
        )(hidden, *w_heads, w_flat)
        n_grp = n_tok // Q_ROWS
        return pl.pallas_call(
            functools.partial(global_layer, n_cp, n_layers - 1, dims),
            out_shape=jax.ShapeDtypeStruct(hidden.shape, hidden.dtype),
            in_specs=[any_spec] * 5, out_specs=any_spec,
            scratch_shapes=[
                vmem((n_tok, d_model), BF16),
                vmem((n_heads, 3, n_tok, head_dim), BF16), vmem((n_cp, 3, n_tok, head_dim), BF16),
                vmem((n_cp, n_tok, head_dim), BF16), vmem((n_tok, width), BF16),
                vmem((2, 3, d_model, head_dim), BF16), vmem((2, width, N_COLS), BF16),
                *[vmem((Q_ROWS, 128), F32)] * (2 * n_grp), *[vmem((Q_ROWS, head_dim), F32)] * n_grp,
                dma, dma((2, 3)), dma((2,)), dma((n_cp,)), dma((n_cp,)), dma((n_cp,)), dma((n_cp,)),
            ],
            compiler_params=pltpu.CompilerParams(collective_id=1, has_side_effects=True, vmem_limit_bytes=big),
            cost_estimate=pl.CostEstimate(flops=8 * flops, bytes_accessed=63 * 2 ** 20, transcendentals=0),
            name="global_layer",
        )(hidden, *w_heads, w_flat)

    row_spec = P(("dp", "cp"), None)
    return jax.shard_map(device_body, mesh=mesh, in_specs=(row_spec, P(), P(), P(), P()), out_specs=row_spec, check_vma=False)
```
